32 devices in a mesh: samp: 4 (over y, x), snp: 8 (over z, core).
Axes of the slice: x: 2, y: 2, z: 4, core: 2. Of those that a mesh axis runs over, the one named last changes fastest.
Arguments:
- genotypes: int32 [8192, 8192], P('samp', 'snp'), may hold values from 0 to 2
- win_lo: int32 [8192], P('snp'), may hold values from 0 to 8191, as said below
- win_hi: int32 [8192], P('snp'), may hold values from 0 to 8191, as said below
- annotation: int32 [8192], P('snp'), may hold values from 0 to 127
- chromosome: int32 [8192], P('snp'), may hold values from 0 to 21, never falling along the last dimension, each value on 1 to 512 neighbouring positions
- chi_square: float32 [8192], P('snp'), may hold values from 0.3 to 60
Outputs:
- annotation_scores: float32 [128, 8192], P('snp')
- gram: float32 [128, 128], replicated
- moments: float32 [2, 128], replicated
- totals: float32 [2], replicated
The draws below stay inside these ranges and needn't reach their ends.
Inputs may be any that keep to these rules, and one draw needn't show every extreme that they name: i - 512 <= win_lo[i] <= i, nondecreasing in i; the distance 512 is reached. i <= win_hi[i] <= i + 512, nondecreasing in i; the distance 512 is reached.
All inputs are finite; a program needn't handle non-finite values.
Results may differ from the reference program's by a relative error of at most 0.0003.
The reference program's roundings to bfloat16 on the way (of `standard`) count: a program that leaves them out, or rounds other values in their place, can miss the bound.
Values may be sent and summed in bfloat16 or wider, within the bound.
A program may use at most 64 MiB of HBM per device.

```python
import math
import jax
import jax.numpy as jnp
import numpy as np
from jax import lax

A = 128
SAMPLES = 8192
SNPS = 8192
REACH = 512


def recomb_rates(key):
    base_key = jax.random.fold_in(key, 7001)
    region = jax.random.randint(jax.random.fold_in(base_key, 1), (SNPS // REACH + 1,), 1, 9)
    extra_rate = jax.random.randint(jax.random.fold_in(base_key, 2), (SNPS,), 0, 2)
    positions = jnp.arange(SNPS, dtype=jnp.int32)
    return (region[positions // REACH] + extra_rate).astype(jnp.int32)


def window_bounds(key):
    rate_steps = recomb_rates(key)
    places = jnp.cumsum(rate_steps).astype(jnp.int32)
    span_units = 3 * REACH
    lower_end = jnp.searchsorted(places, places - span_units, side='left').astype(jnp.int32)
    upper_end = (jnp.searchsorted(places, places + span_units, side='right') - 1).astype(jnp.int32)
    positions = jnp.arange(SNPS, dtype=jnp.int32)
    lower_end = jnp.maximum(lower_end, positions - REACH)
    upper_end = jnp.minimum(upper_end, positions + REACH)
    return (lower_end, upper_end)


def draw_win_lo(key, part):
    return window_bounds(key)[0]


def draw_win_hi(key, part):
    return window_bounds(key)[1]


def draw_genotypes(key, part):
    rate_steps = recomb_rates(key)
    base_key = jax.random.fold_in(key, 7003)
    frequency = jax.random.randint(jax.random.fold_in(base_key, 1), (SNPS,), 50, 500)
    keep_level = jax.random.randint(jax.random.fold_in(base_key, 4), (SNPS,), 500, 1000)
    step_keys = jax.random.split(jax.random.fold_in(base_key, 2), SNPS)
    initial = (jax.random.randint(jax.random.fold_in(base_key, 3), (2, SAMPLES), 0, 1000) < frequency[0]).astype(jnp.int32)

    def advance(haplotype, inputs):
        step_key, allele_level, flip_level, carry_level = inputs
        uniform_draws = jax.random.randint(step_key, (3, 2, SAMPLES), 0, 1000)
        fresh_allele = (uniform_draws[0] < allele_level).astype(jnp.int32)
        haplotype = jnp.where(uniform_draws[1] < flip_level, fresh_allele, haplotype)
        carried = (uniform_draws[2] < carry_level).astype(jnp.int32)
        return (haplotype, jnp.sum(haplotype * carried, 0))
    _, dosage = lax.scan(advance, initial, (step_keys, frequency, rate_steps, keep_level))
    return dosage.T.astype(jnp.int32)


def draw_chi_square(key, part):
    base_key = jax.random.fold_in(key, 7005)
    positions = jnp.arange(SNPS, dtype=jnp.float32)
    ramp = 1.0 + 2.0 * positions / SNPS
    values = jnp.exp(jax.random.uniform(base_key, (SNPS,), jnp.float32, math.log(0.3), math.log(20.0)))
    return (values * ramp).astype(jnp.float32)


def touch_ends(entries, rng, least, high):
    shape = entries.shape
    spot = [jax.random.randint(jax.random.fold_in(rng, axis), (), 0, shape[axis]) for axis in range(len(shape))]
    entries = entries.at[tuple(spot)].set(least)
    longest = shape.index(max(shape))
    spot[longest] = (spot[longest] + 1) % shape[longest]
    return entries.at[tuple(spot)].set(high)


def cumulative_ranks(number_of, lean):
    portions = [(1 << 20) // math.isqrt(rank ** lean) + 1 for rank in range(1, number_of + 1)]
    scale = 1 + sum(portions) // (1 << 30)
    return np.cumsum(np.array([max(1, weight // scale) for weight in portions]))


def ranked(stream_key, extent, number_of, lean):
    table = cumulative_ranks(number_of, lean)
    ticket = jax.random.randint(jax.random.fold_in(stream_key, 1), extent, 0, int(table[number_of - 1]))
    rank = jnp.searchsorted(jnp.asarray(table, jnp.int32), ticket, side="right")
    return jax.random.permutation(jax.random.fold_in(stream_key, 2), number_of)[rank].astype(jnp.int32)


def profile(count, total, limit, slope):
    weights = [(1 << 20) // math.isqrt(rank ** slope) + 1 for rank in range(2, count + 1)]
    surplus, holding = total - limit - (count - 1), [1] * (count - 1)
    while surplus > 0:
        free = [i for i in range(count - 1) if holding[i] < limit]
        whole, budget = sum([weights[i] for i in free]), surplus
        for i in free:
            addition = min(limit - holding[i], max(1, budget * weights[i] // whole), surplus)
            holding[i] = holding[i] + addition
            surplus = surplus - addition
    return np.array([limit] + holding)


def uneven_parts(rng, count, total, limit, lean):
    if count == 2:
        one = jax.random.randint(rng, (), max(1, total - limit), min(limit, total - 1) + 1)
        return jnp.stack([one, total - one])
    sizes = jnp.asarray(profile(count, total, limit, lean), jnp.int32)
    couples = (count - 1) // 2
    giver, sink = sizes[1:1 + 2 * couples:2], sizes[2:2 + 2 * couples:2]
    slack = jnp.minimum(giver - 1, limit - sink)
    shifted = jax.random.randint(jax.random.fold_in(rng, 1), (couples,), 0, 1 << 20) % (slack + 1)
    sizes = sizes.at[1:1 + 2 * couples:2].set(giver - shifted).at[2:2 + 2 * couples:2].set(sink + shifted)
    return sizes[jax.random.permutation(jax.random.fold_in(rng, 2), count)]


def setup_inputs(seed: int = 0) -> dict:
    key_of = jax.random.split(jax.random.key(seed), 7)
    genotypes = draw_genotypes(jax.random.fold_in(key_of[6], 71), 0)
    win_lo = draw_win_lo(jax.random.fold_in(key_of[6], 71), 0)
    win_hi = draw_win_hi(jax.random.fold_in(key_of[6], 71), 0)
    annotation = touch_ends(ranked(key_of[3], (SNPS,), A, 1), jax.random.fold_in(key_of[3], 3), 0, A - 1).astype(jnp.int32)
    chromosome = jnp.searchsorted(jnp.cumsum(uneven_parts(key_of[4], 22, SNPS, SNPS // 16, 1)), jnp.arange(SNPS), side="right").astype(jnp.int32)
    chi_square = draw_chi_square(jax.random.fold_in(key_of[6], 71), 0)
    return dict(genotypes=genotypes, win_lo=win_lo, win_hi=win_hi, annotation=annotation, chromosome=chromosome, chi_square=chi_square)


def reference(genotypes, win_lo, win_hi, annotation, chromosome, chi_square):
    dosage = genotypes.astype(jnp.float32)
    mean_dose = lax.optimization_barrier(jnp.sum(dosage, 0)) / SAMPLES
    variance = lax.optimization_barrier(jnp.sum(dosage * dosage, 0)) / SAMPLES - mean_dose * mean_dose
    standard = ((dosage - mean_dose) * lax.rsqrt(variance + 1e-05)).astype(jnp.bfloat16)
    padded = jnp.pad(standard, ((0, 0), (REACH, REACH)))
    annot_pad = jnp.pad(annotation, REACH)
    chrom_pad = jnp.pad(chromosome, REACH)
    labels = jnp.arange(A, dtype=jnp.int32)

    def one_block(block):
        first_row = (block * REACH).astype(jnp.int32)
        rows_z = lax.dynamic_slice_in_dim(standard, first_row, REACH, 1).astype(jnp.float32)
        cols_z = lax.dynamic_slice_in_dim(padded, first_row, 3 * REACH, 1).astype(jnp.float32)
        tile = lax.dot_general(rows_z, cols_z, (((0,), (0,)), ((), ())), preferred_element_type=jnp.float32)
        corr = tile / SAMPLES
        square = corr * corr
        adjusted = square - (1.0 - square) / (SAMPLES - 2)
        col_ids = first_row - REACH + jnp.arange(3 * REACH, dtype=jnp.int32)
        lower_end = lax.dynamic_slice_in_dim(win_lo, first_row, REACH)
        upper_end = lax.dynamic_slice_in_dim(win_hi, first_row, REACH)
        chrom_rows = lax.dynamic_slice_in_dim(chromosome, first_row, REACH)
        chrom_cols = lax.dynamic_slice_in_dim(chrom_pad, first_row, 3 * REACH)
        annot_cols = lax.dynamic_slice_in_dim(annot_pad, first_row, 3 * REACH)
        inside = (col_ids[None, :] >= lower_end[:, None]) & (col_ids[None, :] <= upper_end[:, None])
        inside = inside & (chrom_cols[None, :] == chrom_rows[:, None])
        kept = jnp.where(inside, adjusted, 0.0)
        member = (annot_cols[:, None] == labels[None, :]).astype(jnp.float32)
        return lax.dot_general(member, kept, (((0,), (1,)), ((), ())), precision=lax.Precision.HIGHEST, preferred_element_type=jnp.float32)
    blocks = lax.map(one_block, jnp.arange(SNPS // REACH, dtype=jnp.int32))
    scores = jnp.transpose(blocks, (1, 0, 2)).reshape(A, SNPS)
    weights = 1.0 / lax.optimization_barrier(jnp.sum(scores, 0))
    weighted = scores * weights[None, :]
    scale = A / SNPS
    gram = scale * lax.dot_general(weighted, scores, (((1,), (1,)), ((), ())), precision=lax.Precision.HIGHEST, preferred_element_type=jnp.float32)
    moments = scale * jnp.stack([lax.optimization_barrier(jnp.sum(weighted, 1)), lax.optimization_barrier(jnp.sum(weighted * chi_square[None, :], 1))])
    totals = jnp.stack([jnp.sum(weights), jnp.sum(weights * chi_square)]) / SNPS
    return (scores, gram, moments, totals)
```

```python
import functools

import jax
import jax.numpy as jnp
from jax import lax
from jax.experimental import pallas as pl
from jax.experimental.pallas import tpu as pltpu
from jax.sharding import PartitionSpec as P

A = 128
EDGE = 32000.0


def remote(src, dst, send_sem, recv_sem, device):
    return pltpu.make_async_remote_copy(
        src_ref=src,
        dst_ref=dst,
        send_sem=send_sem,
        recv_sem=recv_sem,
        device_id=device,
        device_id_type=pl.DeviceIdType.MESH,
    )


def kernel(
    n_samp, n_snp, chunk,
    meta_ref, geno_ref,
    out_ref, gram_ref, small_ref,
    gbuf, zt, wide, labels, stat, stat_all, own, sendq, recvq,
    score_parts, gs_parts, score_in, gs_in, gs_sum, score_all, gs_all, gram_rows, gram_all,
    load_sem, stat_ss, stat_rs, lab_ss, lab_rs, halo_ss, halo_rs, tile_ss, tile_rs,
    a1_ss, a1_rs, a2_ss, a2_rs, b1_ss, b1_rs, b2_ss, b2_rs, c_ss, c_rs,
):
    rows, cols = gbuf.shape
    half = cols // 2
    share = cols // n_samp
    tiles = recvq.shape[1]
    n_chunks = rows // chunk
    group = A // n_snp
    total = rows * n_samp
    steps = EDGE / (total * 1.004)
    s = lax.axis_index("samp")
    p = lax.axis_index("snp")
    has_left = p > 0
    has_right = p < n_snp - 1
    left = jnp.maximum(p - 1, 0)
    right = jnp.minimum(p + 1, n_snp - 1)

    def load(c):
        part = pl.ds(pl.multiple_of(c * chunk, chunk), chunk)
        return pltpu.make_async_copy(geno_ref.at[part], gbuf.at[part], load_sem.at[c])

    for c in range(n_chunks):
        load(c).start()

    barrier = pltpu.get_barrier_semaphore()
    for k in range(1, n_samp):
        pl.semaphore_signal(barrier, inc=1, device_id={"samp": lax.rem(s + k, n_samp)}, device_id_type=pl.DeviceIdType.MESH)

    @pl.loop(1, n_snp)
    def _(k):
        pl.semaphore_signal(barrier, inc=1, device_id={"snp": lax.rem(p + k, n_snp)}, device_id_type=pl.DeviceIdType.MESH)

    pl.semaphore_wait(barrier, n_samp - 1 + n_snp - 1)

    lab_left = remote(meta_ref.at[:, pl.ds(0, half)], labels.at[:, pl.ds(half + cols, half)], lab_ss.at[0], lab_rs.at[0], {"snp": left})
    lab_right = remote(meta_ref.at[:, pl.ds(half, half)], labels.at[:, pl.ds(0, half)], lab_ss.at[1], lab_rs.at[1], {"snp": right})

    @pl.when(has_left)
    def _():
        lab_left.start()

    @pl.when(has_right)
    def _():
        lab_right.start()

    def tally(c, sums):
        load(c).wait()
        one, two = sums
        for b in range(cols // 256):
            g = gbuf[pl.ds(pl.multiple_of(c * chunk, chunk), chunk), b * 256:(b + 1) * 256].astype(jnp.float32)
            g1 = jnp.sum(g.reshape(chunk // 8, 8, 256), 0)
            g2 = jnp.sum((g * g).reshape(chunk // 8, 8, 256), 0)
            one = one[:b] + (one[b] + g1,) + one[b + 1:]
            two = two[:b] + (two[b] + g2,) + two[b + 1:]
        return one, two

    blank = tuple(jnp.zeros((8, 256), jnp.float32) for _ in range(cols // 256))
    one, two = lax.fori_loop(0, n_chunks, tally, (blank, blank))
    for b in range(cols // 256):
        stat[0:1, b * 256:(b + 1) * 256] = jnp.sum(one[b], 0, keepdims=True)
        stat[1:2, b * 256:(b + 1) * 256] = jnp.sum(two[b], 0, keepdims=True)

    def stat_copy(k):
        return remote(stat, stat_all.at[k - 1], stat_ss.at[k - 1], stat_rs.at[k - 1], {"samp": lax.rem(s + k, n_samp)})

    for k in range(1, n_samp):
        stat_copy(k).start()
    labels[:, half:half + cols] = meta_ref[...]

    @pl.when(jnp.logical_not(has_left))
    def _():
        wide[:, 0:half] = jnp.zeros((rows, half), jnp.bfloat16)
        labels[:, 0:half] = jnp.full((8, half), -1.0, jnp.float32)

    @pl.when(jnp.logical_not(has_right))
    def _():
        wide[:, half + cols:] = jnp.zeros((rows, half), jnp.bfloat16)
        labels[:, half + cols:] = jnp.full((8, half), -1.0, jnp.float32)

    sums = stat[...]
    for k in range(1, n_samp):
        stat_copy(k).wait()
        sums = sums + stat_all[k - 1]
    mean = sums[0:1] / total
    scale = lax.rsqrt(sums[1:2] / total - mean * mean + 1e-05)

    def halo_left(c):
        part = pl.ds(pl.multiple_of(c * chunk, chunk), chunk)
        return remote(wide.at[part, pl.ds(half, half)], wide.at[part, pl.ds(half + cols, half)], halo_ss.at[0, c], halo_rs.at[0, c], {"snp": left})

    def halo_right(c):
        part = pl.ds(pl.multiple_of(c * chunk, chunk), chunk)
        return remote(wide.at[part, pl.ds(cols, half)], wide.at[part, pl.ds(0, half)], halo_ss.at[1, c], halo_rs.at[1, c], {"snp": right})

    def halo_start(c):
        @pl.when(has_left)
        def _():
            halo_left(c).start()

        @pl.when(has_right)
        def _():
            halo_right(c).start()

    @pl.loop(0, n_chunks)
    def _(c):
        start = pl.multiple_of(c * chunk, chunk)
        for b in range(cols // 256):
            at = slice(b * 256, (b + 1) * 256)
            g = gbuf[pl.ds(start, chunk), at].astype(jnp.float32)
            z = (g - mean[:, at]) * scale[:, at]
            wide[pl.ds(start, chunk), half + b * 256:half + (b + 1) * 256] = z.astype(jnp.bfloat16)
            zt[at, pl.ds(start, chunk)] = z.T.astype(jnp.bfloat16)

        halo_start(c)

    def tile_copy(k, t):
        return remote(sendq.at[k - 1, t], recvq.at[k - 1, t], tile_ss.at[k - 1, t], tile_rs.at[k - 1, t], {"samp": lax.rem(s + k, n_samp)})

    def tile_pass(inner):
        @pl.loop(0, n_samp * tiles)
        def _(step):
            k = lax.rem(step // tiles + 1, n_samp)
            t = lax.rem(step, tiles)
            r = lax.rem(s + k, n_samp)
            at = r * share + t * share
            inside = jnp.logical_and(at >= half, at < half + cols)

            @pl.when(inside if inner else jnp.logical_not(inside))
            def _():
                part = jnp.dot(
                    zt[pl.ds(pl.multiple_of(r * share, share), share), :],
                    wide[:, pl.ds(pl.multiple_of(at, share), share)],
                    preferred_element_type=jnp.float32,
                )

                @pl.when(k == 0)
                def _():
                    own[t] = part

                @pl.when(k > 0)
                def _():
                    fixed = jnp.clip(jnp.round(part * steps), -32767.0, 32767.0)
                    sendq[k - 1, t] = fixed.astype(jnp.int32).astype(jnp.int16)
                    tile_copy(k, t).start()

    tile_pass(True)

    @pl.when(has_left)
    def _():
        lab_left.wait_send()
        lab_right.wait_recv()

        @pl.loop(0, n_chunks)
        def _(c):
            halo_left(c).wait_send()
            halo_right(c).wait_recv()

    @pl.when(has_right)
    def _():
        lab_right.wait_send()
        lab_left.wait_recv()

        @pl.loop(0, n_chunks)
        def _(c):
            halo_right(c).wait_send()
            halo_left(c).wait_recv()

    tile_pass(False)

    mine = pl.multiple_of(s * share, share)
    info = meta_ref[:, pl.ds(mine, share)]
    turned = jnp.concatenate([info] + [jnp.zeros((A - 8, share), jnp.float32)], 0).T
    lower, upper, chrom = turned[:, 0:1], turned[:, 1:2], turned[:, 2:3]
    chi = info[4:5]
    first = (p * cols - half).astype(jnp.int32)

    def add_tile(t, scores):
        tile = own[t]
        got = jnp.zeros((share, share), jnp.float32)
        for k in range(1, n_samp):
            tile_copy(k, t).wait()
            got = got + recvq[k - 1, t].astype(jnp.int32).astype(jnp.float32)
        corr = (tile + got * (1.0 / steps)) / total
        square = corr * corr
        adjusted = square - (1.0 - square) / (total - 2)
        at = pl.multiple_of((s + t) * share, share)
        lab = labels[:, pl.ds(at, share)]
        ids = (first + at + lax.broadcasted_iota(jnp.int32, (1, share), 1)).astype(jnp.float32)
        inside = (ids >= lower) & (ids <= upper) & (lab[2:3] == chrom)
        kept = jnp.where(inside, adjusted, 0.0)
        cats = lax.broadcasted_iota(jnp.int32, (A, share), 0).astype(jnp.float32)
        member = jnp.where(cats == lab[3:4], 1.0, 0.0).astype(jnp.bfloat16)
        for _ in range(3):
            piece = kept.astype(jnp.bfloat16)
            kept = kept - piece.astype(jnp.float32)
            scores = scores + lax.dot_general(member, piece, (((1,), (1,)), ((), ())), preferred_element_type=jnp.float32)
        return scores

    scores = lax.fori_loop(0, tiles, add_tile, jnp.zeros((A, share), jnp.float32))

    weights = 1.0 / jnp.sum(scores, 0, keepdims=True)
    weighted = scores * weights
    gram = lax.dot_general(
        weighted, scores, (((1,), (1,)), ((), ())), precision=lax.Precision.HIGHEST, preferred_element_type=jnp.float32
    )
    for q in range(n_snp):
        score_parts[q] = scores[q * group:(q + 1) * group]
    pair = jnp.concatenate([weights, weights * chi, jnp.zeros((6, share), jnp.float32)], 0)
    moments = lax.dot_general(
        pair, scores, (((1,), (1,)), ((), ())), precision=lax.Precision.HIGHEST, preferred_element_type=jnp.float32
    )
    sums2 = jnp.broadcast_to(jnp.sum(pair, 1, keepdims=True), (8, A))
    for q in range(n_snp):
        gs_parts[q, 0:8] = jnp.concatenate([moments[0:2], sums2[0:2], moments[4:8]], 0)
        gs_parts[q, 8:8 + group] = gram[q * group:(q + 1) * group]

    def send_gs(k):
        q = lax.rem(p + k, n_snp)
        return remote(gs_parts.at[q], gs_in.at[k], a1_ss.at[k], a1_rs.at[k], {"snp": q})

    def send_scores(k):
        q = lax.rem(p + k, n_snp)
        return remote(score_parts.at[q], score_in.at[p], a2_ss.at[k], a2_rs.at[k], {"snp": q})

    @pl.loop(1, n_snp)
    def _(k):
        send_gs(k).start()

    @pl.loop(1, n_snp)
    def _(k):
        send_scores(k).start()

    score_in[p] = score_parts[p]

    def add_gs(k, so_far):
        send_gs(k).wait()
        return so_far + gs_in[k]

    gs_sum[...] = lax.fori_loop(1, n_snp, add_gs, gs_parts[p])

    def share_gs(k):
        return remote(gs_sum, gs_all.at[k - 1], b1_ss.at[k - 1], b1_rs.at[k - 1], {"samp": lax.rem(s + k, n_samp)})

    def share_scores(k):
        return remote(score_in, score_all.at[s], b2_ss.at[k - 1], b2_rs.at[k - 1], {"samp": lax.rem(s + k, n_samp)})

    for k in range(1, n_samp):
        share_gs(k).start()

    @pl.loop(1, n_snp)
    def _(k):
        send_scores(k).wait()

    for k in range(1, n_samp):
        share_scores(k).start()
    score_all[s] = score_in[...]

    full = gs_sum[...]
    for k in range(1, n_samp):
        share_gs(k).wait()
        full = full + gs_all[k - 1]
    gram_rows[...] = full[8:8 + group]
    factor = A / (cols * n_snp)
    small_ref[...] = full[0:8]

    def send_rows(k):
        return remote(gram_rows, gram_all.at[p], c_ss.at[k], c_rs.at[k], {"snp": lax.rem(p + k, n_snp)})

    @pl.loop(1, n_snp)
    def _(k):
        send_rows(k).start()

    gram_all[p] = gram_rows[...]

    @pl.loop(1, n_snp)
    def _(k):
        send_rows(k).wait()

    for q in range(n_snp):
        gram_ref[q * group:(q + 1) * group, :] = gram_all[q] * factor
    for k in range(1, n_samp):
        share_scores(k).wait()
    for r in range(n_samp):
        for q in range(n_snp):
            start = q * cols + r * share
            out_ref[:, start:start + share] = score_all[r, q]


def solution(mesh):
    n_samp, n_snp = mesh.shape["samp"], mesh.shape["snp"]

    def body(genotypes, win_lo, win_hi, annotation, chromosome, chi_square):
        rows, cols = genotypes.shape
        half, share = cols // 2, cols // n_samp
        chunk = 256
        n_chunks = rows // chunk
        tiles = (cols + share) // share
        group = A // n_snp
        as_row = lambda x: x.astype(jnp.float32)
        nothing = jnp.zeros((cols,), jnp.float32)
        meta = jnp.stack(
            [as_row(win_lo), as_row(win_hi), as_row(chromosome), as_row(annotation), chi_square, nothing, nothing, nothing]
        )
        f32, bf16, i16 = jnp.float32, jnp.bfloat16, jnp.int16
        dma = pltpu.SemaphoreType.DMA
        out, gram, small = pl.pallas_call(
            functools.partial(kernel, n_samp, n_snp, chunk),
            out_shape=(
                jax.ShapeDtypeStruct((group, cols * n_snp), f32),
                jax.ShapeDtypeStruct((A, A), f32),
                jax.ShapeDtypeStruct((8, A), f32),
            ),
            in_specs=[pl.BlockSpec(memory_space=pltpu.VMEM), pl.BlockSpec(memory_space=pl.ANY)],
            out_specs=(pl.BlockSpec(memory_space=pltpu.VMEM),) * 3,
            scratch_shapes=[
                pltpu.VMEM((rows, cols), jnp.int32),
                pltpu.VMEM((cols, rows), bf16),
                pltpu.VMEM((rows, 2 * cols), bf16),
                pltpu.VMEM((8, 2 * cols), f32),
                pltpu.VMEM((2, cols), f32),
                pltpu.VMEM((n_samp - 1, 2, cols), f32),
                pltpu.VMEM((tiles, share, share), f32),
                pltpu.VMEM((n_samp - 1, tiles, share, share), i16),
                pltpu.VMEM((n_samp - 1, tiles, share, share), i16),
                pltpu.VMEM((n_snp, group, share), f32),
                pltpu.VMEM((n_snp, group + 8, A), f32),
                pltpu.VMEM((n_snp, group, share), f32),
                pltpu.VMEM((n_snp, group + 8, A), f32),
                pltpu.VMEM((group + 8, A), f32),
                pltpu.VMEM((n_samp, n_snp, group, share), f32),
                pltpu.VMEM((n_samp - 1, group + 8, A), f32),
                pltpu.VMEM((group, A), f32),
                pltpu.VMEM((n_snp, group, A), f32),
                dma((n_chunks,)),
                dma((n_samp - 1,)), dma((n_samp - 1,)),
                dma((2,)), dma((2,)),
                dma((2, n_chunks)), dma((2, n_chunks)),
                dma((n_samp - 1, tiles)), dma((n_samp - 1, tiles)),
                dma((n_snp,)), dma((n_snp,)),
                dma((n_snp,)), dma((n_snp,)),
                dma((n_samp - 1,)), dma((n_samp - 1,)),
                dma((n_samp - 1,)), dma((n_samp - 1,)),
                dma((n_snp,)), dma((n_snp,)),
            ],
            compiler_params=pltpu.CompilerParams(
                collective_id=0, has_side_effects=True, vmem_limit_bytes=60 * 1024 * 1024
            ),
        )(meta, genotypes)
        snps = cols * n_snp
        return out, gram, small[0:2] * (A / snps), small[2:4, 0] / snps

    in_specs = (P("samp", "snp"), P("snp"), P("snp"), P("snp"), P("snp"), P("snp"))
    out_specs = (P("snp", None), P(), P(), P())
    return jax.shard_map(body, mesh=mesh, in_specs=in_specs, out_specs=out_specs, check_vma=False)
```

```python
import functools

import jax
import jax.numpy as jnp
from jax import lax
from jax.experimental import pallas as pl
from jax.experimental.pallas import tpu as pltpu
from jax.sharding import PartitionSpec as P

A = 128
EDGE = 32000.0


def remote(src, dst, send_sem, recv_sem, device):
    return pltpu.make_async_remote_copy(
        src_ref=src,
        dst_ref=dst,
        send_sem=send_sem,
        recv_sem=recv_sem,
        device_id=device,
        device_id_type=pl.DeviceIdType.MESH,
    )


def kernel(
    n_samp, n_snp, chunk,
    meta_ref, geno_ref,
    out_ref, gram_ref, small_ref,
    gbuf, zt, wide, labels, stat, stat_all, own, sendq, recvq, fwd_out, fwd_in,
    score_parts, gs_parts, score_in, gs_in, gs_sum, score_all, gs_all, gram_rows, gram_all,
    load_sem, stat_ss, stat_rs, lab_ss, lab_rs, halo_ss, halo_rs, tile_ss, tile_rs, fwd_ss, fwd_rs,
    a1_ss, a1_rs, a2_ss, a2_rs, b1_ss, b1_rs, b2_ss, b2_rs, c_ss, c_rs,
):
    rows, cols = gbuf.shape
    half = cols // 2
    share = cols // n_samp
    n_chunks = rows // chunk
    group = A // n_snp
    total = rows * n_samp
    steps = EDGE / (total * 1.004)
    s = lax.axis_index("samp")
    p = lax.axis_index("snp")
    has_left = p > 0
    has_right = p < n_snp - 1
    left = jnp.maximum(p - 1, 0)
    right = jnp.minimum(p + 1, n_snp - 1)

    def load(c):
        part = pl.ds(pl.multiple_of(c * chunk, chunk), chunk)
        return pltpu.make_async_copy(geno_ref.at[part], gbuf.at[part], load_sem.at[c])

    for c in range(n_chunks):
        load(c).start()

    barrier = pltpu.get_barrier_semaphore()
    for k in range(1, n_samp):
        pl.semaphore_signal(barrier, inc=1, device_id={"samp": lax.rem(s + k, n_samp)}, device_id_type=pl.DeviceIdType.MESH)

    @pl.loop(1, n_snp)
    def _(k):
        pl.semaphore_signal(barrier, inc=1, device_id={"snp": lax.rem(p + k, n_snp)}, device_id_type=pl.DeviceIdType.MESH)

    @pl.when(has_left)
    def _():
        for k in range(1, n_samp):
            pl.semaphore_signal(barrier, inc=1, device_id={"samp": lax.rem(s + k, n_samp), "snp": left}, device_id_type=pl.DeviceIdType.MESH)

    @pl.when(has_right)
    def _():
        for k in range(1, n_samp):
            pl.semaphore_signal(barrier, inc=1, device_id={"samp": lax.rem(s + k, n_samp), "snp": right}, device_id_type=pl.DeviceIdType.MESH)

    pl.semaphore_wait(barrier, n_samp - 1 + n_snp - 1 + (n_samp - 1) * (right - left))

    lab_left = remote(meta_ref.at[:, pl.ds(0, half)], labels.at[:, pl.ds(half + cols, half)], lab_ss.at[0], lab_rs.at[0], {"snp": left})
    lab_right = remote(meta_ref.at[:, pl.ds(half, half)], labels.at[:, pl.ds(0, half)], lab_ss.at[1], lab_rs.at[1], {"snp": right})

    @pl.when(has_left)
    def _():
        lab_left.start()

    @pl.when(has_right)
    def _():
        lab_right.start()

    def tally(c, sums):
        load(c).wait()
        one, two = sums
        for b in range(cols // 256):
            g = gbuf[pl.ds(pl.multiple_of(c * chunk, chunk), chunk), b * 256:(b + 1) * 256].astype(jnp.float32)
            g1 = jnp.sum(g.reshape(chunk // 8, 8, 256), 0)
            g2 = jnp.sum((g * g).reshape(chunk // 8, 8, 256), 0)
            one = one[:b] + (one[b] + g1,) + one[b + 1:]
            two = two[:b] + (two[b] + g2,) + two[b + 1:]
        return one, two

    blank = tuple(jnp.zeros((8, 256), jnp.float32) for _ in range(cols // 256))
    one, two = lax.fori_loop(0, n_chunks, tally, (blank, blank))
    for b in range(cols // 256):
        stat[0:1, b * 256:(b + 1) * 256] = jnp.sum(one[b], 0, keepdims=True)
        stat[1:2, b * 256:(b + 1) * 256] = jnp.sum(two[b], 0, keepdims=True)

    def stat_copy(k):
        return remote(stat, stat_all.at[k - 1], stat_ss.at[k - 1], stat_rs.at[k - 1], {"samp": lax.rem(s + k, n_samp)})

    for k in range(1, n_samp):
        stat_copy(k).start()
    labels[:, half:half + cols] = meta_ref[...]

    @pl.when(jnp.logical_not(has_left))
    def _():
        wide[:, 0:share] = jnp.zeros((rows, share), jnp.bfloat16)
        labels[:, 0:half] = jnp.full((8, half), -1.0, jnp.float32)

    @pl.when(jnp.logical_not(has_right))
    def _():
        wide[:, share + cols:] = jnp.zeros((rows, share), jnp.bfloat16)
        labels[:, half + cols:] = jnp.full((8, half), -1.0, jnp.float32)

    sums = stat[...]
    for k in range(1, n_samp):
        stat_copy(k).wait()
        sums = sums + stat_all[k - 1]
    mean = sums[0:1] / total
    scale = lax.rsqrt(sums[1:2] / total - mean * mean + 1e-05)

    def halo_left(c):
        part = pl.ds(pl.multiple_of(c * chunk, chunk), chunk)
        return remote(wide.at[part, pl.ds(share, share)], wide.at[part, pl.ds(share + cols, share)], halo_ss.at[0, c], halo_rs.at[0, c], {"snp": left})

    def halo_right(c):
        part = pl.ds(pl.multiple_of(c * chunk, chunk), chunk)
        return remote(wide.at[part, pl.ds(cols, share)], wide.at[part, pl.ds(0, share)], halo_ss.at[1, c], halo_rs.at[1, c], {"snp": right})

    def halo_start(c):
        @pl.when(has_left)
        def _():
            halo_left(c).start()

        @pl.when(has_right)
        def _():
            halo_right(c).start()

    @pl.loop(0, n_chunks)
    def _(c):
        start = pl.multiple_of(c * chunk, chunk)
        for b in range(cols // 256):
            at = slice(b * 256, (b + 1) * 256)
            g = gbuf[pl.ds(start, chunk), at].astype(jnp.float32)
            z = (g - mean[:, at]) * scale[:, at]
            wide[pl.ds(start, chunk), share + b * 256:share + (b + 1) * 256] = z.astype(jnp.bfloat16)
            zt[at, pl.ds(start, chunk)] = z.T.astype(jnp.bfloat16)

        halo_start(c)

    def tile_copy(k, t):
        return remote(sendq.at[k - 1, t], recvq.at[k - 1, t], tile_ss.at[k - 1, t], tile_rs.at[k - 1, t], {"samp": lax.rem(s + k, n_samp)})

    def column(r, u):
        odd, high = lax.rem(r, 2), r // 2
        second = 2 - 3 * odd + high * (2 + 3 * odd)
        return (r if u == 0 else 1 + lax.rem(r, 3)) if u < 2 else second

    def tile_pass(u, inner):
        @pl.loop(0, n_samp)
        def _(step):
            k = lax.rem(step + 1, n_samp)
            r = lax.rem(s + k, n_samp)

            def work():
                part = jnp.dot(
                    zt[pl.ds(pl.multiple_of(r * share, share), share), :],
                    wide[:, pl.ds(pl.multiple_of((column(r, u) + 1) * share, share), share)],
                    preferred_element_type=jnp.float32,
                )

                @pl.when(k == 0)
                def _():
                    own[u] = part

                @pl.when(k > 0)
                def _():
                    sendq[k - 1, u] = to_fixed(part)
                    tile_copy(k, u).start()

            if u < 2:
                work()
            else:
                pl.when(r == 0 if inner else r > 0)(work)

    def to_fixed(part):
        return jnp.clip(jnp.round(part * steps), -32767.0, 32767.0).astype(jnp.int32).astype(jnp.int16)

    def from_fixed(tile):
        return tile.astype(jnp.int32).astype(jnp.float32)

    def total_tile(u):
        got = jnp.zeros((share, share), jnp.float32)
        for k in range(1, n_samp):
            tile_copy(k, u).wait()
            got = got + from_fixed(recvq[k - 1, u])
        return own[u] + got * (1.0 / steps)

    slot = lax.rem(s, 2)
    high = s // 2
    step_to = high - slot * (1 - high)
    near = {"samp": 1 + lax.rem(s, 3)}
    far = {"samp": (2 + s) * (1 - high), "snp": jnp.clip(p + step_to, 0, n_snp - 1)}
    far_there = jnp.logical_and(p + step_to >= 0, p + step_to < n_snp)
    forward = (
        remote(fwd_out.at[0], fwd_in.at[slot], fwd_ss.at[0], fwd_rs.at[slot], near),
        remote(fwd_out.at[1], fwd_in.at[slot], fwd_ss.at[1], fwd_rs.at[slot], far),
    )

    tile_pass(1, True)
    tile_pass(2, True)
    tile_pass(0, True)

    @pl.when(has_left)
    def _():
        lab_left.wait_send()
        lab_right.wait_recv()

        @pl.loop(0, n_chunks)
        def _(c):
            halo_left(c).wait_send()
            halo_right(c).wait_recv()

    @pl.when(has_right)
    def _():
        lab_right.wait_send()
        lab_left.wait_recv()

        @pl.loop(0, n_chunks)
        def _(c):
            halo_right(c).wait_send()
            halo_left(c).wait_recv()

    tile_pass(2, False)

    one_sum = total_tile(1)
    own[1] = one_sum
    fwd_out[0] = to_fixed(one_sum)
    forward[0].start()
    mine = pl.multiple_of(s * share, share)
    info = meta_ref[:, pl.ds(mine, share)]
    turned = jnp.concatenate([info] + [jnp.zeros((A - 8, share), jnp.float32)], 0).T
    lower, upper, chrom = turned[:, 0:1], turned[:, 1:2], turned[:, 2:3]
    chi = info[4:5]
    first = (p * cols - half).astype(jnp.int32)

    def add_tile(tile, block, scores):
        corr = tile / total
        square = corr * corr
        adjusted = square - (1.0 - square) / (total - 2)
        at = pl.multiple_of(block * share + half, share)
        lab = labels[:, pl.ds(at, share)]
        ids = (first + at + lax.broadcasted_iota(jnp.int32, (1, share), 1)).astype(jnp.float32)
        inside = (ids >= lower) & (ids <= upper) & (lab[2:3] == chrom)
        kept = jnp.where(inside, adjusted, 0.0)
        cats = lax.broadcasted_iota(jnp.int32, (A, share), 0).astype(jnp.float32)
        member = jnp.where(cats == lab[3:4], 1.0, 0.0).astype(jnp.bfloat16)
        for _ in range(2):
            piece = kept.astype(jnp.bfloat16)
            kept = kept - piece.astype(jnp.float32)
            scores = scores + lax.dot_general(member, piece, (((1,), (1,)), ((), ())), preferred_element_type=jnp.float32)
        return scores

    scores = add_tile(total_tile(0), s, jnp.zeros((A, share), jnp.float32))
    two_sum = total_tile(2)
    fwd_out[1] = to_fixed(two_sum)

    @pl.when(far_there)
    def _():
        forward[1].start()

    scores = add_tile(two_sum, column(s, 2), scores)
    scores = add_tile(own[1], column(s, 1), scores)
    forward[0].wait_send()

    @pl.when(far_there)
    def _():
        forward[1].wait_send()

    for i in range(2):
        arrives = jnp.logical_and(jnp.logical_or(s > 0, has_left), jnp.logical_or(s < n_samp - i, has_right))
        got = remote(fwd_out.at[i], fwd_in.at[i], fwd_ss.at[i], fwd_rs.at[i], near)

        @pl.when(arrives)
        def _():
            got.wait_recv()

        @pl.when(jnp.logical_not(arrives))
        def _():
            fwd_in[i] = jnp.zeros((share, share), jnp.int16)

        block = 2 * ((s + 1) // 2) - 2 + i * (1 + 2 * lax.rem(s, 2))
        scores = add_tile(from_fixed(fwd_in[i]).T * (1.0 / steps), block, scores)

    weights = 1.0 / jnp.sum(scores, 0, keepdims=True)
    weighted = scores * weights
    gram = lax.dot_general(
        weighted, scores, (((1,), (1,)), ((), ())), precision=lax.Precision.HIGHEST, preferred_element_type=jnp.float32
    )
    for q in range(n_snp):
        score_parts[q] = scores[q * group:(q + 1) * group]
    pair = jnp.concatenate([weights, weights * chi, jnp.zeros((6, share), jnp.float32)], 0)
    moments = lax.dot_general(
        pair, scores, (((1,), (1,)), ((), ())), precision=lax.Precision.HIGHEST, preferred_element_type=jnp.float32
    )
    sums2 = jnp.broadcast_to(jnp.sum(pair, 1, keepdims=True), (8, A))
    for q in range(n_snp):
        gs_parts[q, 0:8] = jnp.concatenate([moments[0:2], sums2[0:2], moments[4:8]], 0)
        gs_parts[q, 8:8 + group] = gram[q * group:(q + 1) * group]

    def send_gs(k):
        q = lax.rem(p + k, n_snp)
        return remote(gs_parts.at[q], gs_in.at[k], a1_ss.at[k], a1_rs.at[k], {"snp": q})

    def send_scores(k):
        q = lax.rem(p + k, n_snp)
        return remote(score_parts.at[q], score_in.at[p], a2_ss.at[k], a2_rs.at[k], {"snp": q})

    @pl.loop(1, n_snp)
    def _(k):
        send_gs(k).start()

    @pl.loop(1, n_snp)
    def _(k):
        send_scores(k).start()

    score_in[p] = score_parts[p]

    def add_gs(k, so_far):
        send_gs(k).wait()
        return so_far + gs_in[k]

    gs_sum[...] = lax.fori_loop(1, n_snp, add_gs, gs_parts[p])

    def share_gs(k):
        return remote(gs_sum, gs_all.at[k - 1], b1_ss.at[k - 1], b1_rs.at[k - 1], {"samp": lax.rem(s + k, n_samp)})

    def share_scores(k):
        return remote(score_in, score_all.at[s], b2_ss.at[k - 1], b2_rs.at[k - 1], {"samp": lax.rem(s + k, n_samp)})

    for k in range(1, n_samp):
        share_gs(k).start()

    @pl.loop(1, n_snp)
    def _(k):
        send_scores(k).wait()

    for k in range(1, n_samp):
        share_scores(k).start()
    score_all[s] = score_in[...]

    full = gs_sum[...]
    for k in range(1, n_samp):
        share_gs(k).wait()
        full = full + gs_all[k - 1]
    gram_rows[...] = full[8:8 + group]
    factor = A / (cols * n_snp)
    small_ref[...] = full[0:8]

    def send_rows(k):
        return remote(gram_rows, gram_all.at[p], c_ss.at[k], c_rs.at[k], {"snp": lax.rem(p + k, n_snp)})

    @pl.loop(1, n_snp)
    def _(k):
        send_rows(k).start()

    gram_all[p] = gram_rows[...]

    @pl.loop(1, n_snp)
    def _(k):
        send_rows(k).wait()

    for q in range(n_snp):
        gram_ref[q * group:(q + 1) * group, :] = gram_all[q] * factor
    for k in range(1, n_samp):
        share_scores(k).wait()
    for r in range(n_samp):
        for q in range(n_snp):
            start = q * cols + r * share
            out_ref[:, start:start + share] = score_all[r, q]


def solution(mesh):
    n_samp, n_snp = mesh.shape["samp"], mesh.shape["snp"]

    def body(genotypes, win_lo, win_hi, annotation, chromosome, chi_square):
        rows, cols = genotypes.shape
        half, share = cols // 2, cols // n_samp
        chunk = 256
        n_chunks = rows // chunk
        tiles = 3
        group = A // n_snp
        as_row = lambda x: x.astype(jnp.float32)
        nothing = jnp.zeros((cols,), jnp.float32)
        meta = jnp.stack(
            [as_row(win_lo), as_row(win_hi), as_row(chromosome), as_row(annotation), chi_square, nothing, nothing, nothing]
        )
        f32, bf16, i16 = jnp.float32, jnp.bfloat16, jnp.int16
        dma = pltpu.SemaphoreType.DMA
        out, gram, small = pl.pallas_call(
            functools.partial(kernel, n_samp, n_snp, chunk),
            out_shape=(
                jax.ShapeDtypeStruct((group, cols * n_snp), f32),
                jax.ShapeDtypeStruct((A, A), f32),
                jax.ShapeDtypeStruct((8, A), f32),
            ),
            in_specs=[pl.BlockSpec(memory_space=pltpu.VMEM), pl.BlockSpec(memory_space=pl.ANY)],
            out_specs=(pl.BlockSpec(memory_space=pltpu.VMEM),) * 3,
            scratch_shapes=[
                pltpu.VMEM((rows, cols), jnp.int32),
                pltpu.VMEM((cols, rows), bf16),
                pltpu.VMEM((rows, cols + 2 * share), bf16),
                pltpu.VMEM((8, 2 * cols), f32),
                pltpu.VMEM((2, cols), f32),
                pltpu.VMEM((n_samp - 1, 2, cols), f32),
                pltpu.VMEM((tiles, share, share), f32),
                pltpu.VMEM((n_samp - 1, tiles, share, share), i16),
                pltpu.VMEM((n_samp - 1, tiles, share, share), i16),
                pltpu.VMEM((2, share, share), i16),
                pltpu.VMEM((2, share, share), i16),
                pltpu.VMEM((n_snp, group, share), f32),
                pltpu.VMEM((n_snp, group + 8, A), f32),
                pltpu.VMEM((n_snp, group, share), f32),
                pltpu.VMEM((n_snp, group + 8, A), f32),
                pltpu.VMEM((group + 8, A), f32),
                pltpu.VMEM((n_samp, n_snp, group, share), f32),
                pltpu.VMEM((n_samp - 1, group + 8, A), f32),
                pltpu.VMEM((group, A), f32),
                pltpu.VMEM((n_snp, group, A), f32),
                dma((n_chunks,)),
                dma((n_samp - 1,)), dma((n_samp - 1,)),
                dma((2,)), dma((2,)),
                dma((2, n_chunks)), dma((2, n_chunks)),
                dma((n_samp - 1, tiles)), dma((n_samp - 1, tiles)),
                dma((2,)), dma((2,)),
                dma((n_snp,)), dma((n_snp,)),
                dma((n_snp,)), dma((n_snp,)),
                dma((n_samp - 1,)), dma((n_samp - 1,)),
                dma((n_samp - 1,)), dma((n_samp - 1,)),
                dma((n_snp,)), dma((n_snp,)),
            ],
            compiler_params=pltpu.CompilerParams(
                collective_id=0, has_side_effects=True, vmem_limit_bytes=60 * 1024 * 1024
            ),
        )(meta, genotypes)
        snps = cols * n_snp
        return out, gram, small[0:2] * (A / snps), small[2:4, 0] / snps

    in_specs = (P("samp", "snp"), P("snp"), P("snp"), P("snp"), P("snp"), P("snp"))
    out_specs = (P("snp", None), P(), P(), P())
    return jax.shard_map(body, mesh=mesh, in_specs=in_specs, out_specs=out_specs, check_vma=False)
```
